32 devices in a mesh: vblk: 4 (over y, x), samp: 8 (over z, core).
Axes of the slice: x: 2, y: 2, z: 4, core: 2. Of those that a mesh axis runs over, the one named last changes fastest.
Arguments:
- vectors: bfloat16 [1024, 32768], P('vblk', 'samp'), may hold values from 0 to 2, as said below
- partner: bfloat16 [1024, 32768], P('vblk', 'samp'), may hold values from 0 to 2, as said below
- next_rows: bfloat16 [1024, 32768], P(('vblk', 'samp')), may hold values from 0 to 2, as said below
Outputs:
- metric: float32 [1024, 256], P('vblk', 'samp')
- next_block: bfloat16 [1024, 32768], P('vblk', 'samp')
The draws below stay inside these ranges and needn't reach their ends.
Inputs may be any that keep to these rules, and one draw needn't show every extreme that they name: vectors: real expected allele dosages, every entry positive. partner: real expected allele dosages, every entry positive. next_rows: real expected allele dosages, every entry positive.
All inputs are finite; a program needn't handle non-finite values.
Results may differ from the reference program's by a relative error of at most 0.0004.
Values may be sent and summed in bfloat16 or wider, within the bound.
A program may use at most 64 MiB of HBM per device.

```python
import math
import jax
import jax.numpy as jnp
from jax import lax

NSAMP = 32768
NVD = 256
NVEC = 1024
NXVEC = 1024
N_VBLK = 4
N_SAMP = 8


def shard_factor(key, salt_value, low_value):
    key = jax.random.fold_in(key, salt_value)
    factors = jnp.exp(jax.random.uniform(key, (N_SAMP,), jnp.float32, math.log(low_value), 0.0))
    return jnp.repeat(factors, NSAMP // N_SAMP)[None, :]


def dosage(key, salt_value, row_count):
    common = shard_factor(key, 20, 1.0 / 30.0)
    if salt_value == 13:
        own_factor = jnp.ones((1, NSAMP), jnp.float32)
    else:
        own_factor = shard_factor(key, 20 + salt_value, 0.03)
    key = jax.random.fold_in(key, salt_value)
    subkeys = jax.random.split(key, 3)
    low = math.log(0.1)
    row_scale = jnp.exp(jax.random.uniform(subkeys[0], (row_count, 1), jnp.float32, low, 0.0))
    sample_ramp = (1.0 + 2.0 * jnp.arange(NSAMP, dtype=jnp.float32) / (NSAMP - 1)) / 3.0
    col_scale = jnp.exp(jax.random.uniform(subkeys[1], (1, NSAMP), jnp.float32, low, 0.0)) * sample_ramp[None, :]
    col_scale = col_scale * common * own_factor
    raw_values = jax.random.uniform(subkeys[2], (row_count, NSAMP), jnp.float32, 0.05, 1.0)
    return (2.0 * row_scale * col_scale * raw_values).astype(jnp.bfloat16)


def draw_vectors(key, part):
    return dosage(key, 11, NVEC)


def draw_partner(key, part):
    return dosage(key, 12, NVEC)


def draw_next_rows(key, part):
    return dosage(key, 13, NXVEC)


def setup_inputs(seed: int = 0) -> dict:
    arg_keys = jax.random.split(jax.random.key(seed), 4)
    return {
        "vectors": draw_vectors(jax.random.fold_in(arg_keys[3], 71), 0),
        "partner": draw_partner(jax.random.fold_in(arg_keys[3], 71), 0),
        "next_rows": draw_next_rows(jax.random.fold_in(arg_keys[3], 71), 0),
    }


def block_metric(own_block, pair_block):
    row_count = own_block.shape[0]
    grouped = own_block.reshape(row_count // 8, 8, own_block.shape[1])
    pair_wide = pair_block.astype(jnp.float32)

    def group_sums(row_group):
        return jnp.sum(jnp.minimum(row_group.astype(jnp.float32)[:, None, :], pair_wide[None, :, :]), axis=2)

    numerators = lax.map(group_sums, grouped).reshape(row_count, pair_block.shape[0])
    own_totals = jnp.sum(own_block.astype(jnp.float32), axis=1)
    pair_totals = jnp.sum(pair_wide, axis=1)
    return 2.0 * numerators / (own_totals[:, None] + pair_totals[None, :])


def reference(vectors, partner, next_rows):
    own_blocks = vectors.reshape(N_VBLK, NVD, NSAMP)
    pair_blocks = jnp.roll(partner.reshape(N_VBLK, NVD, NSAMP), 1, axis=0)
    metric = lax.map(lambda paired: block_metric(paired[0], paired[1]), (own_blocks, pair_blocks))
    return metric.reshape(NVEC, NVD), next_rows
```

```python
import functools

import jax
import jax.numpy as jnp
from jax import lax
from jax.experimental import pallas as pl
from jax.experimental.pallas import tpu as pltpu
from jax.sharding import PartitionSpec as P

MESH = pl.DeviceIdType.MESH
SUB = 8
ALIGN = 16
WIDTH = 256
UNROLL = 8
TREE = 8
KTILE = 256
ROWS_PER_DOT = 256
VMEM_BYTES = 60 * 1024 * 1024


def from_behind(value, axis, steps):
    count = lax.axis_size(axis)
    pairs = [(source, (source + steps) % count) for source in range(count)]
    return lax.ppermute(value, axis, pairs)


def pair_terms(row_block, col_block):
    row_count = row_block.shape[0]
    grouped = row_block.reshape(row_count // 8, 8, row_block.shape[1])

    def group_sums(row_group):
        return jnp.sum(
            jnp.minimum(row_group[:, None, :], col_block[None, :, :]), axis=2, dtype=jnp.float32
        )

    numerators = lax.map(group_sums, grouped).reshape(row_count, col_block.shape[0])
    row_totals = jnp.sum(row_block, axis=1, dtype=jnp.float32)[:, None]
    col_totals = jnp.sum(col_block, axis=1, dtype=jnp.float32)[None, :]
    return (numerators, row_totals, col_totals)


def plain_body(vectors, partner, next_rows):
    next_block = lax.all_to_all(next_rows, "samp", split_axis=1, concat_axis=0, tiled=True)
    arrived = from_behind(partner, "vblk", 1)
    numerators, row_totals, col_totals = pair_terms(vectors, arrived)
    numerators, col_totals = (
        lax.psum_scatter(numerators, "samp", scatter_dimension=1, tiled=True),
        lax.psum_scatter(col_totals, "samp", scatter_dimension=1, tiled=True),
    )
    row_totals = lax.psum(row_totals, "samp")
    metric = 2.0 * numerators / (row_totals + col_totals)
    return (metric, next_block)


def flipped(index, mask, count):
    out = 0
    bit = 1
    while bit < count:
        out = out + lax.rem(lax.div(index, bit) + lax.div(mask, bit), 2) * bit
        bit *= 2
    return out


def tree_sum(values):
    while len(values) > 1:
        values = [values[i] + values[i + 1] for i in range(0, len(values), 2)]
    return values[0]


def row_sums(block):
    ones = jnp.ones((8, block.shape[1]), jnp.bfloat16)
    return lax.dot_general(
        ones, block, (((1,), (1,)), ((), ())), preferred_element_type=jnp.float32
    )


def spread(slot, count):
    out = 0
    bit = 1
    while bit < count:
        out = out + lax.rem(lax.div(slot, bit), 2) * (count // (2 * bit))
        bit *= 2
    return out


def kernel(
    n_vblk, n_samp,
    vec_hbm, partner_hbm, next_hbm,
    total_ref, block_hbm,
    vec, wide, arrived, own_piece, part, part_in,
    vec_sem, piece_sem, go_sem, pair_send, pair_recv, next_send, next_recv, part_send, part_recv,
):
    b = lax.axis_index("vblk")
    s = lax.axis_index("samp")
    up = lax.rem(b + 1, n_vblk)
    down = lax.rem(b + n_vblk - 1, n_vblk)
    odd = lax.rem(s, 2)
    row_count, samples = vec.shape
    cols = row_count // n_samp
    next_count = next_hbm.shape[0]
    group = ROWS_PER_DOT // cols
    span = TREE * KTILE
    units = samples // span

    vec_copy = pltpu.make_async_copy(vec_hbm, vec, vec_sem)
    vec_copy.start()
    own_in = pltpu.make_async_copy(
        next_hbm.at[:, pl.ds(pl.multiple_of(s * samples, samples), samples)],
        own_piece, piece_sem.at[0],
    )
    own_in.start()

    barrier = pltpu.get_barrier_semaphore()
    pl.semaphore_signal(barrier, inc=1, device_id=(down, s), device_id_type=MESH)
    for peer in range(1, n_samp, 2):
        @pl.when(s != peer)
        def _():
            pl.semaphore_signal(barrier, inc=1, device_id=(b, peer), device_id_type=MESH)
    pl.semaphore_wait(barrier, 1 + odd * (n_samp - 1))

    def pair_copy(x, u):
        owner = flipped(s, spread(x, n_samp), n_samp)
        return pltpu.make_async_remote_copy(
            src_ref=partner_hbm.at[
                pl.ds(pl.multiple_of(owner * cols, cols), cols), pl.ds(u * span, span)
            ],
            dst_ref=arrived.at[x, :, pl.ds(u * span, span)],
            send_sem=pair_send.at[x * units + u], recv_sem=pair_recv.at[x * units + u],
            device_id=(up, s), device_id_type=MESH,
        )

    def next_copy(m):
        peer = flipped(s, m, n_samp)
        return pltpu.make_async_remote_copy(
            src_ref=next_hbm.at[:, pl.ds(pl.multiple_of(peer * samples, samples), samples)],
            dst_ref=block_hbm.at[pl.ds(pl.multiple_of(s * next_count, next_count), next_count), :],
            send_sem=next_send.at[m], recv_sem=next_recv.at[m],
            device_id=(b, peer), device_id_type=MESH,
        )

    def part_copy(x, mask):
        return pltpu.make_async_remote_copy(
            src_ref=part.at[x], dst_ref=part_in.at[x],
            send_sem=part_send.at[x], recv_sem=part_recv.at[x],
            device_id=(b, flipped(s, mask, n_samp)), device_id_type=MESH,
        )

    for x in reversed(range(n_samp)):
        for u in range(units):
            pair_copy(x, u).start()

    @pl.when(odd == 1)
    def _():
        pl.semaphore_signal(go_sem, inc=1, device_id=(b, s - 1), device_id_type=MESH)

    @pl.when(odd == 0)
    def _():
        pl.semaphore_wait(go_sem, 1)

    for m in range(1, n_samp):
        next_copy(m).start()

    own_in.wait()
    own_out = pltpu.make_async_copy(
        own_piece,
        block_hbm.at[pl.ds(pl.multiple_of(s * next_count, next_count), next_count), :],
        piece_sem.at[1],
    )
    own_out.start()

    vec_copy.wait()

    def widen(t, carry):
        first = pl.multiple_of(t * ALIGN, ALIGN)
        for c in range(samples // WIDTH):
            lanes = pl.ds(c * WIDTH, WIDTH)
            rows = vec[pl.ds(first, ALIGN), lanes].astype(jnp.float32)
            for r in range(ALIGN):
                wide[first + r, :, lanes] = jnp.broadcast_to(
                    rows[r:r + 1, :], (SUB, WIDTH)
                ).astype(jnp.bfloat16)
        return carry

    lax.fori_loop(0, row_count // ALIGN, widen, 0)

    own_totals = row_sums(vec[:, pl.ds(0, KTILE)])
    own_totals = lax.fori_loop(
        1, samples // KTILE,
        lambda k, acc: acc + row_sums(vec[:, pl.ds(pl.multiple_of(k * KTILE, KTILE), KTILE)]),
        own_totals,
    )

    groups = row_count // group

    def chunk(i, carry):
        x = n_samp - 1 - i
        for u in range(units):
            pair_copy(x, u).wait_recv()
            at = [pl.ds(u * span + g * KTILE, KTILE) for g in range(TREE)]

            def one_group(q):
                pieces = {}
                for half in range(2):
                    js = range(half * cols // SUB // 2, (half + 1) * cols // SUB // 2)
                    theirs = {j: [arrived[x, pl.ds(j * SUB, SUB), o] for o in at] for j in js}
                    for r in range(group):
                        mine = [wide[r * groups + q, :, o] for o in at]
                        for j in js:
                            pieces[r, j] = tree_sum(
                                [jnp.minimum(v, w) for v, w in zip(mine, theirs[j])]
                            )
                minima = jnp.stack([pieces[key] for key in sorted(pieces)])
                sums = row_sums(minima.reshape(ROWS_PER_DOT, KTILE))[0:1, :]
                if u:
                    sums = sums + part[x, pl.ds(q, 1), :]
                part[x, pl.ds(q, 1), :] = sums

            def groups_step(q, c):
                for k in range(UNROLL):
                    one_group(q * UNROLL + k)
                return c

            lax.fori_loop(0, groups // UNROLL, groups_step, 0)
        part[x, pl.ds(groups, 8), :] = own_totals
        part[x, pl.ds(groups + 1, 1), pl.ds(0, cols)] = row_sums(arrived[x])[0:1, :]

        bit = n_samp // 2
        while bit:
            @pl.when(x < bit)
            def _(bit=bit):
                part_copy(x + bit, n_samp // (2 * bit)).wait_recv()
                part[x] = part[x] + part_in[x + bit]
            bit //= 2
        bit = n_samp // 2
        while bit:
            @pl.when((x >= bit) & (x < 2 * bit))
            def _(bit=bit):
                part_copy(x, n_samp // (2 * bit)).start()
            bit //= 2
        return carry

    lax.fori_loop(0, n_samp, chunk, 0)
    total_ref[...] = part[0]

    for x in range(n_samp):
        for u in range(units):
            pair_copy(x, u).wait_send()
    for x in range(1, n_samp):
        part_copy(x, 1).wait_send()
    for m in range(1, n_samp):
        next_copy(m).wait()
    own_out.wait()


def finish(
    groups, cols, total_hbm, block_in, metric_hbm, block_out,
    total_ref, metric_ref, pieces, in_sems, out_sems, end_sems,
):
    count, rows, _ = pieces.shape

    def take(i):
        return pltpu.make_async_copy(
            block_in.at[pl.ds(i * rows, rows), :], pieces.at[i], in_sems.at[i]
        )

    def give(i):
        return pltpu.make_async_copy(
            pieces.at[i], block_out.at[pl.ds(i * rows, rows), :], out_sems.at[i]
        )

    total_in = pltpu.make_async_copy(total_hbm, total_ref, end_sems.at[0])
    metric_out = pltpu.make_async_copy(metric_ref, metric_hbm, end_sems.at[1])
    total_in.start()
    for i in range(count):
        take(i).start()
    total_in.wait()
    turned = total_ref[pl.ds(0, groups), :].T
    numerators = jnp.concatenate(
        [turned[first:first + cols, :] for first in range(0, turned.shape[0], cols)], axis=1
    )
    own_totals = total_ref[pl.ds(groups, 1), :]
    pair_totals = total_ref[pl.ds(groups, 8), :].T[:cols, 1:2]
    metric_ref[...] = 2.0 * numerators / (own_totals + pair_totals)
    metric_out.start()
    for i in range(count):
        take(i).wait()
        give(i).start()
    for i in range(count):
        give(i).wait()
    metric_out.wait()


def fused_body(n_vblk, n_samp, vectors, partner, next_rows):
    rows, samples = vectors.shape
    cols = rows // n_samp
    groups = rows * cols // ROWS_PER_DOT
    units = samples // (TREE * KTILE)
    part_rows = groups + 8
    next_count = next_rows.shape[0]
    hbm = pl.BlockSpec(memory_space=pl.ANY)
    dma = pltpu.SemaphoreType.DMA
    total, next_block = pl.pallas_call(
        functools.partial(kernel, n_vblk, n_samp),
        out_shape=(
            jax.ShapeDtypeStruct((part_rows, ROWS_PER_DOT), jnp.float32),
            jax.ShapeDtypeStruct((next_count * n_samp, samples), next_rows.dtype),
        ),
        in_specs=[hbm, hbm, hbm],
        out_specs=(pl.BlockSpec(memory_space=pltpu.VMEM), hbm),
        scratch_shapes=[
            pltpu.VMEM((rows, samples), jnp.bfloat16),
            pltpu.VMEM((rows, SUB, samples), jnp.bfloat16),
            pltpu.VMEM((n_samp, cols, samples), jnp.bfloat16),
            pltpu.VMEM((next_count, samples), jnp.bfloat16),
            pltpu.VMEM((n_samp, part_rows, ROWS_PER_DOT), jnp.float32),
            pltpu.VMEM((n_samp, part_rows, ROWS_PER_DOT), jnp.float32),
            dma, dma((2,)), pltpu.SemaphoreType.REGULAR,
            dma((n_samp * units,)), dma((n_samp * units,)),
            dma((n_samp,)), dma((n_samp,)),
            dma((n_samp,)), dma((n_samp,)),
        ],
        compiler_params=pltpu.CompilerParams(
            collective_id=0, has_side_effects=True, vmem_limit_bytes=VMEM_BYTES
        ),
        name="similarity",
    )(vectors, partner, next_rows)
    metric, next_block = pl.pallas_call(
        functools.partial(finish, groups, cols),
        out_shape=(
            jax.ShapeDtypeStruct((cols, rows), jnp.float32),
            jax.ShapeDtypeStruct(next_block.shape, next_block.dtype),
        ),
        in_specs=[hbm, hbm],
        out_specs=(hbm, hbm),
        scratch_shapes=[
            pltpu.VMEM((part_rows, ROWS_PER_DOT), jnp.float32),
            pltpu.VMEM((cols, rows), jnp.float32),
            pltpu.VMEM((n_samp, next_count, samples), next_rows.dtype),
            dma((n_samp,)), dma((n_samp,)), dma((2,)),
        ],
        name="finish",
    )(total, next_block)
    return (metric.T, next_block)


def body(n_vblk, n_samp, vectors, partner, next_rows):
    rows, samples = vectors.shape
    cols = rows // n_samp
    fits = (
        n_vblk > 2
        and n_samp > 1
        and n_samp & (n_samp - 1) == 0
        and rows == ROWS_PER_DOT
        and cols % ALIGN == 0
        and cols % UNROLL == 0
        and samples % (TREE * KTILE) == 0
        and next_rows.shape[0] % ALIGN == 0
        and rows * SUB * samples * 2 + 4 * rows * samples * 2 <= VMEM_BYTES
        and next_rows.shape[0] * n_samp == rows
    )
    if fits:
        return fused_body(n_vblk, n_samp, vectors, partner, next_rows)
    return plain_body(vectors, partner, next_rows)


def solution(mesh):
    in_specs = (P("vblk", "samp"), P("vblk", "samp"), P(("vblk", "samp"), None))
    out_specs = (P("vblk", "samp"), P("vblk", "samp"))
    step = functools.partial(body, mesh.shape["vblk"], mesh.shape["samp"])
    return jax.shard_map(step, mesh=mesh, in_specs=in_specs, out_specs=out_specs, check_vma=False)
```

```python
import functools

import jax
import jax.numpy as jnp
from jax import lax
from jax.experimental import pallas as pl
from jax.experimental.pallas import tpu as pltpu
from jax.sharding import PartitionSpec as P

MESH = pl.DeviceIdType.MESH
SUB = 8
ALIGN = 16
WIDTH = 256
UNROLL = 32
TREE = 8
KTILE = 256
ROWS_PER_DOT = 256
VMEM_BYTES = 60 * 1024 * 1024
KERNEL_BYTES = 51712 * 1024


def from_behind(value, axis, steps):
    count = lax.axis_size(axis)
    pairs = [(source, (source + steps) % count) for source in range(count)]
    return lax.ppermute(value, axis, pairs)


def pair_terms(row_block, col_block):
    row_count = row_block.shape[0]
    grouped = row_block.reshape(row_count // 8, 8, row_block.shape[1])

    def group_sums(row_group):
        return jnp.sum(
            jnp.minimum(row_group[:, None, :], col_block[None, :, :]), axis=2, dtype=jnp.float32
        )

    numerators = lax.map(group_sums, grouped).reshape(row_count, col_block.shape[0])
    row_totals = jnp.sum(row_block, axis=1, dtype=jnp.float32)[:, None]
    col_totals = jnp.sum(col_block, axis=1, dtype=jnp.float32)[None, :]
    return (numerators, row_totals, col_totals)


def plain_body(vectors, partner, next_rows):
    next_block = lax.all_to_all(next_rows, "samp", split_axis=1, concat_axis=0, tiled=True)
    arrived = from_behind(partner, "vblk", 1)
    numerators, row_totals, col_totals = pair_terms(vectors, arrived)
    numerators, col_totals = (
        lax.psum_scatter(numerators, "samp", scatter_dimension=1, tiled=True),
        lax.psum_scatter(col_totals, "samp", scatter_dimension=1, tiled=True),
    )
    row_totals = lax.psum(row_totals, "samp")
    metric = 2.0 * numerators / (row_totals + col_totals)
    return (metric, next_block)


def flipped(index, mask, count):
    out = 0
    bit = 1
    while bit < count:
        out = out + lax.rem(lax.div(index, bit) + lax.div(mask, bit), 2) * bit
        bit *= 2
    return out


def tree_sum(values):
    while len(values) > 1:
        values = [values[i] + values[i + 1] for i in range(0, len(values), 2)]
    return values[0]


def row_sums(block):
    ones = jnp.ones((8, block.shape[1]), jnp.bfloat16)
    return lax.dot_general(
        ones, block, (((1,), (1,)), ((), ())), preferred_element_type=jnp.float32
    )


def spread(slot, count):
    out = 0
    bit = 1
    while bit < count:
        out = out + lax.rem(lax.div(slot, bit), 2) * (count // (2 * bit))
        bit *= 2
    return out


def kernel(
    n_vblk, n_samp,
    vec_hbm, partner_hbm, next_hbm,
    total_ref, block_hbm,
    vec, wide, arrived, own_piece, part, part_in,
    vec_sem, piece_sem, go_sem, pair_send, pair_recv, next_send, next_recv, part_send, part_recv,
):
    b = lax.axis_index("vblk")
    s = lax.axis_index("samp")
    up = lax.rem(b + 1, n_vblk)
    down = lax.rem(b + n_vblk - 1, n_vblk)
    odd = lax.rem(s, 2)
    row_count, samples = vec.shape
    cols = row_count // n_samp
    next_count = next_hbm.shape[0]
    group = ROWS_PER_DOT // cols
    span = TREE * KTILE
    units = samples // span

    vec_copy = pltpu.make_async_copy(vec_hbm, vec, vec_sem)
    vec_copy.start()
    own_in = pltpu.make_async_copy(
        next_hbm.at[:, pl.ds(pl.multiple_of(s * samples, samples), samples)],
        own_piece, piece_sem.at[0],
    )
    own_in.start()

    barrier = pltpu.get_barrier_semaphore()
    pl.semaphore_signal(barrier, inc=1, device_id=(down, s), device_id_type=MESH)
    for peer in range(1, n_samp, 2):
        @pl.when(s != peer)
        def _():
            pl.semaphore_signal(barrier, inc=1, device_id=(b, peer), device_id_type=MESH)
    pl.semaphore_wait(barrier, 1 + odd * (n_samp - 1))

    def pair_copy(x, u):
        owner = flipped(s, spread(x, n_samp), n_samp)
        return pltpu.make_async_remote_copy(
            src_ref=partner_hbm.at[
                pl.ds(pl.multiple_of(owner * cols, cols), cols), pl.ds(u * span, span)
            ],
            dst_ref=arrived.at[x, :, pl.ds(u * span, span)],
            send_sem=pair_send.at[x * units + u], recv_sem=pair_recv.at[x * units + u],
            device_id=(up, s), device_id_type=MESH,
        )

    def next_copy(m):
        peer = flipped(s, m, n_samp)
        return pltpu.make_async_remote_copy(
            src_ref=next_hbm.at[:, pl.ds(pl.multiple_of(peer * samples, samples), samples)],
            dst_ref=block_hbm.at[pl.ds(pl.multiple_of(s * next_count, next_count), next_count), :],
            send_sem=next_send.at[m], recv_sem=next_recv.at[m],
            device_id=(b, peer), device_id_type=MESH,
        )

    def part_copy(x, mask):
        return pltpu.make_async_remote_copy(
            src_ref=part.at[x], dst_ref=part_in.at[x],
            send_sem=part_send.at[x], recv_sem=part_recv.at[x],
            device_id=(b, flipped(s, mask, n_samp)), device_id_type=MESH,
        )

    for x in reversed(range(n_samp)):
        for u in range(units):
            pair_copy(x, u).start()

    @pl.when(odd == 1)
    def _():
        pl.semaphore_signal(go_sem, inc=1, device_id=(b, s - 1), device_id_type=MESH)

    @pl.when(odd == 0)
    def _():
        pl.semaphore_wait(go_sem, 1)

    for m in range(1, n_samp):
        next_copy(m).start()

    own_in.wait()
    own_out = pltpu.make_async_copy(
        own_piece,
        block_hbm.at[pl.ds(pl.multiple_of(s * next_count, next_count), next_count), :],
        piece_sem.at[1],
    )
    own_out.start()

    vec_copy.wait()

    def widen(t, carry):
        first = pl.multiple_of(t * ALIGN, ALIGN)
        for c in range(samples // WIDTH):
            lanes = pl.ds(c * WIDTH, WIDTH)
            rows = vec[pl.ds(first, ALIGN), lanes].astype(jnp.float32)
            for r in range(ALIGN):
                wide[first + r, :, lanes] = jnp.broadcast_to(
                    rows[r:r + 1, :], (SUB, WIDTH)
                ).astype(jnp.bfloat16)
        return carry

    lax.fori_loop(0, row_count // ALIGN, widen, 0)

    own_totals = row_sums(vec[:, pl.ds(0, KTILE)])
    own_totals = lax.fori_loop(
        1, samples // KTILE,
        lambda k, acc: acc + row_sums(vec[:, pl.ds(pl.multiple_of(k * KTILE, KTILE), KTILE)]),
        own_totals,
    )

    groups = row_count // group

    def chunk(i, carry):
        x = n_samp - 1 - i
        for u in range(units):
            pair_copy(x, u).wait_recv()
            at = [pl.ds(u * span + g * KTILE, KTILE) for g in range(TREE)]

            def one_group(q):
                pieces = {}
                for half in range(2):
                    js = range(half * cols // SUB // 2, (half + 1) * cols // SUB // 2)
                    theirs = {j: [arrived[x, pl.ds(j * SUB, SUB), o] for o in at] for j in js}
                    for r in range(group):
                        mine = [wide[r * groups + q, :, o] for o in at]
                        for j in js:
                            pieces[r, j] = tree_sum(
                                [jnp.minimum(v, w) for v, w in zip(mine, theirs[j])]
                            )
                minima = jnp.stack([pieces[key] for key in sorted(pieces)])
                sums = row_sums(minima.reshape(ROWS_PER_DOT, KTILE))[0:1, :]
                if u:
                    sums = sums + part[x, pl.ds(q, 1), :]
                part[x, pl.ds(q, 1), :] = sums

            def groups_step(q, c):
                for k in range(UNROLL):
                    one_group(q * UNROLL + k)
                return c

            lax.fori_loop(0, groups // UNROLL, groups_step, 0)
        part[x, pl.ds(groups, 8), :] = own_totals
        part[x, pl.ds(groups + 1, 1), pl.ds(0, cols)] = row_sums(arrived[x])[0:1, :]

        bit = n_samp // 2
        while bit:
            @pl.when(x < bit)
            def _(bit=bit):
                part_copy(x + bit, n_samp // (2 * bit)).wait_recv()
                part[x] = part[x] + part_in[x + bit]
            bit //= 2
        bit = n_samp // 2
        while bit:
            @pl.when((x >= bit) & (x < 2 * bit))
            def _(bit=bit):
                part_copy(x, n_samp // (2 * bit)).start()
            bit //= 2
        return carry

    lax.fori_loop(0, n_samp, chunk, 0)
    total_ref[...] = part[0]

    for x in range(n_samp):
        for u in range(units):
            pair_copy(x, u).wait_send()
    for x in range(1, n_samp):
        part_copy(x, 1).wait_send()
    for m in range(1, n_samp):
        next_copy(m).wait()
    own_out.wait()


def finish(
    groups, cols, total_ref, block_in, metric_hbm, block_out, metric_ref, end_sems,
):
    block_copy = pltpu.make_async_copy(block_in, block_out, end_sems.at[0])
    metric_copy = pltpu.make_async_copy(metric_ref, metric_hbm, end_sems.at[1])
    block_copy.start()
    turned = total_ref[pl.ds(0, groups), :].T
    numerators = jnp.concatenate(
        [turned[first:first + cols, :] for first in range(0, turned.shape[0], cols)], axis=1
    )
    own_totals = total_ref[pl.ds(groups, 1), :]
    pair_totals = total_ref[pl.ds(groups, 8), :].T[:cols, 1:2]
    metric_ref[...] = 2.0 * numerators / (own_totals + pair_totals)
    metric_copy.start()
    block_copy.wait()
    metric_copy.wait()


def fused_body(n_vblk, n_samp, vectors, partner, next_rows):
    rows, samples = vectors.shape
    cols = rows // n_samp
    groups = rows * cols // ROWS_PER_DOT
    units = samples // (TREE * KTILE)
    part_rows = groups + 8
    next_count = next_rows.shape[0]
    hbm = pl.BlockSpec(memory_space=pl.ANY)
    dma = pltpu.SemaphoreType.DMA
    total, next_block = pl.pallas_call(
        functools.partial(kernel, n_vblk, n_samp),
        out_shape=(
            jax.ShapeDtypeStruct((part_rows, ROWS_PER_DOT), jnp.float32),
            jax.ShapeDtypeStruct((next_count * n_samp, samples), next_rows.dtype),
        ),
        in_specs=[pl.BlockSpec(memory_space=pltpu.HBM)] * 3,
        out_specs=(pl.BlockSpec(memory_space=pltpu.VMEM), hbm),
        scratch_shapes=[
            pltpu.VMEM((rows, samples), jnp.bfloat16),
            pltpu.VMEM((rows, SUB, samples), jnp.bfloat16),
            pltpu.VMEM((n_samp, cols, samples), jnp.bfloat16),
            pltpu.VMEM((next_count, samples), jnp.bfloat16),
            pltpu.VMEM((n_samp, part_rows, ROWS_PER_DOT), jnp.float32),
            pltpu.VMEM((n_samp, part_rows, ROWS_PER_DOT), jnp.float32),
            dma, dma((2,)), pltpu.SemaphoreType.REGULAR,
            dma((n_samp * units,)), dma((n_samp * units,)),
            dma((n_samp,)), dma((n_samp,)),
            dma((n_samp,)), dma((n_samp,)),
        ],
        compiler_params=pltpu.CompilerParams(
            collective_id=0, has_side_effects=True, vmem_limit_bytes=KERNEL_BYTES
        ),
        name="similarity",
    )(vectors, partner, next_rows)
    metric, next_block = pl.pallas_call(
        functools.partial(finish, groups, cols),
        out_shape=(
            jax.ShapeDtypeStruct((cols, rows), jnp.float32),
            jax.ShapeDtypeStruct(next_block.shape, next_block.dtype),
        ),
        in_specs=[pl.BlockSpec(memory_space=pltpu.VMEM)] * 2,
        out_specs=(hbm, hbm),
        scratch_shapes=[pltpu.VMEM((cols, rows), jnp.float32), dma((2,))],
        compiler_params=pltpu.CompilerParams(vmem_limit_bytes=8 * 1024 * 1024),
        name="finish",
    )(total, next_block)
    return (metric.T, next_block)


def body(n_vblk, n_samp, vectors, partner, next_rows):
    rows, samples = vectors.shape
    cols = rows // n_samp
    fits = (
        n_vblk > 2
        and n_samp > 1
        and n_samp & (n_samp - 1) == 0
        and rows == ROWS_PER_DOT
        and cols % ALIGN == 0
        and (rows * cols // ROWS_PER_DOT) % UNROLL == 0
        and samples % (TREE * KTILE) == 0
        and next_rows.shape[0] % ALIGN == 0
        and rows * SUB * samples * 2 + 4 * rows * samples * 2 <= VMEM_BYTES
        and next_rows.shape[0] * n_samp == rows
    )
    if fits:
        return fused_body(n_vblk, n_samp, vectors, partner, next_rows)
    return plain_body(vectors, partner, next_rows)


def solution(mesh):
    in_specs = (P("vblk", "samp"), P("vblk", "samp"), P(("vblk", "samp"), None))
    out_specs = (P("vblk", "samp"), P("vblk", "samp"))
    step = functools.partial(body, mesh.shape["vblk"], mesh.shape["samp"])
    return jax.shard_map(step, mesh=mesh, in_specs=in_specs, out_specs=out_specs, check_vma=False)
```

```python
import functools

import jax
import jax.numpy as jnp
from jax import lax
from jax.experimental import pallas as pl
from jax.experimental.pallas import tpu as pltpu
from jax.sharding import PartitionSpec as P

MESH = pl.DeviceIdType.MESH
SUB = 8
ALIGN = 16
WIDTH = 256
TREE = 8
TAIL_TREE = 4
KTILE = 256
ROWS_PER_DOT = 256
VMEM_BYTES = 60 * 1024 * 1024
KERNEL_BYTES = 51712 * 1024


def from_behind(value, axis, steps):
    count = lax.axis_size(axis)
    pairs = [(source, (source + steps) % count) for source in range(count)]
    return lax.ppermute(value, axis, pairs)


def pair_terms(row_block, col_block):
    row_count = row_block.shape[0]
    grouped = row_block.reshape(row_count // 8, 8, row_block.shape[1])

    def group_sums(row_group):
        return jnp.sum(
            jnp.minimum(row_group[:, None, :], col_block[None, :, :]), axis=2, dtype=jnp.float32
        )

    numerators = lax.map(group_sums, grouped).reshape(row_count, col_block.shape[0])
    row_totals = jnp.sum(row_block, axis=1, dtype=jnp.float32)[:, None]
    col_totals = jnp.sum(col_block, axis=1, dtype=jnp.float32)[None, :]
    return (numerators, row_totals, col_totals)


def plain_body(vectors, partner, next_rows):
    next_block = lax.all_to_all(next_rows, "samp", split_axis=1, concat_axis=0, tiled=True)
    arrived = from_behind(partner, "vblk", 1)
    numerators, row_totals, col_totals = pair_terms(vectors, arrived)
    numerators, col_totals = (
        lax.psum_scatter(numerators, "samp", scatter_dimension=1, tiled=True),
        lax.psum_scatter(col_totals, "samp", scatter_dimension=1, tiled=True),
    )
    row_totals = lax.psum(row_totals, "samp")
    metric = 2.0 * numerators / (row_totals + col_totals)
    return (metric, next_block)


def flipped(index, mask, count):
    out = 0
    bit = 1
    while bit < count:
        out = out + lax.rem(lax.div(index, bit) + lax.div(mask, bit), 2) * bit
        bit *= 2
    return out


def tree_sum(values):
    while len(values) > 1:
        values = [values[i] + values[i + 1] for i in range(0, len(values), 2)]
    return values[0]


def row_sums(block, ones=None):
    if ones is None:
        ones = jnp.ones((SUB, block.shape[1]), jnp.bfloat16)
    return lax.dot_general(
        ones, block, (((1,), (1,)), ((), ())), preferred_element_type=jnp.float32
    )


def spread(slot, count):
    out = 0
    bit = 1
    while bit < count:
        out = out + lax.rem(lax.div(slot, bit), 2) * (count // (2 * bit))
        bit *= 2
    return out


def kernel(
    n_vblk, n_samp,
    vec_hbm, partner_hbm, next_hbm,
    total_ref, block_hbm,
    vec, wide, arrived, own_piece, part, part_in,
    vec_sem, piece_sem, go_sem, pair_send, pair_recv, next_send, next_recv, part_send, part_recv,
):
    b = lax.axis_index("vblk")
    s = lax.axis_index("samp")
    up = lax.rem(b + 1, n_vblk)
    down = lax.rem(b + n_vblk - 1, n_vblk)
    odd = lax.rem(s, 2)
    row_count, samples = vec.shape
    cols = row_count // n_samp
    next_count = next_hbm.shape[0]
    group = ROWS_PER_DOT // cols
    span = TAIL_TREE * KTILE
    units = samples // span

    vec_copy = pltpu.make_async_copy(vec_hbm, vec, vec_sem)
    vec_copy.start()
    own_in = pltpu.make_async_copy(
        next_hbm.at[:, pl.ds(pl.multiple_of(s * samples, samples), samples)],
        own_piece, piece_sem.at[0],
    )
    own_in.start()

    barrier = pltpu.get_barrier_semaphore()
    pl.semaphore_signal(barrier, inc=1, device_id=(down, s), device_id_type=MESH)
    for peer in range(1, n_samp, 2):
        @pl.when(s != peer)
        def _():
            pl.semaphore_signal(barrier, inc=1, device_id=(b, peer), device_id_type=MESH)
    pl.semaphore_wait(barrier, 1 + odd * (n_samp - 1))

    def pair_copy(x, u):
        owner = flipped(s, spread(x, n_samp), n_samp)
        return pltpu.make_async_remote_copy(
            src_ref=partner_hbm.at[
                pl.ds(pl.multiple_of(owner * cols, cols), cols), pl.ds(u * span, span)
            ],
            dst_ref=arrived.at[x, :, pl.ds(u * span, span)],
            send_sem=pair_send.at[x * units + u], recv_sem=pair_recv.at[x * units + u],
            device_id=(up, s), device_id_type=MESH,
        )

    def next_copy(m):
        peer = flipped(s, m, n_samp)
        return pltpu.make_async_remote_copy(
            src_ref=next_hbm.at[:, pl.ds(pl.multiple_of(peer * samples, samples), samples)],
            dst_ref=block_hbm.at[pl.ds(pl.multiple_of(s * next_count, next_count), next_count), :],
            send_sem=next_send.at[m], recv_sem=next_recv.at[m],
            device_id=(b, peer), device_id_type=MESH,
        )

    def part_copy(x, mask):
        return pltpu.make_async_remote_copy(
            src_ref=part.at[x], dst_ref=part_in.at[x],
            send_sem=part_send.at[x], recv_sem=part_recv.at[x],
            device_id=(b, flipped(s, mask, n_samp)), device_id_type=MESH,
        )

    def start_pairs(chunks):
        for x in chunks:
            for u in range(units):
                pair_copy(x, u).start()

    held = n_samp // 4
    start_pairs(reversed(range(held, n_samp)))
    pl.when(odd == 1)(functools.partial(start_pairs, reversed(range(held))))

    @pl.when(odd == 1)
    def _():
        pl.semaphore_signal(go_sem, inc=1, device_id=(b, s - 1), device_id_type=MESH)

    @pl.when(odd == 0)
    def _():
        pl.semaphore_wait(go_sem, 1)

    for m in range(1, n_samp):
        next_copy(m).start()

    own_in.wait()
    own_out = pltpu.make_async_copy(
        own_piece,
        block_hbm.at[pl.ds(pl.multiple_of(s * next_count, next_count), next_count), :],
        piece_sem.at[1],
    )
    own_out.start()

    vec_copy.wait()

    def widen(t, carry):
        first = pl.multiple_of(t * ALIGN, ALIGN)
        for c in range(samples // WIDTH):
            lanes = pl.ds(c * WIDTH, WIDTH)
            rows = vec[pl.ds(first, ALIGN), lanes].astype(jnp.float32)
            for r in range(ALIGN):
                wide[first + r, :, lanes] = jnp.broadcast_to(
                    rows[r:r + 1, :], (SUB, WIDTH)
                ).astype(jnp.bfloat16)
        return carry

    lax.fori_loop(0, row_count // ALIGN, widen, 0)

    own_totals = row_sums(vec[:, pl.ds(0, KTILE)])
    own_totals = lax.fori_loop(
        1, samples // KTILE,
        lambda k, acc: acc + row_sums(vec[:, pl.ds(pl.multiple_of(k * KTILE, KTILE), KTILE)]),
        own_totals,
    )

    groups = row_count // group

    rows_of = lax.broadcasted_iota(jnp.int32, (SUB, KTILE), 0)
    one_row = [(rows_of == k).astype(jnp.bfloat16) for k in range(SUB)]

    def add_unit(x, first, tree):
        for u in range(first // span, (first + tree * KTILE) // span):
            pair_copy(x, u).wait_recv()
        at = [pl.ds(first + g * KTILE, KTILE) for g in range(tree)]

        def one_group(q):
            pieces = {}
            for half in range(2):
                js = range(half * cols // SUB // 2, (half + 1) * cols // SUB // 2)
                theirs = {j: [arrived[x, pl.ds(j * SUB, SUB), o] for o in at] for j in js}
                for r in range(group):
                    mine = [wide[r * groups + q, :, o] for o in at]
                    for j in js:
                        pieces[r, j] = tree_sum(
                            [jnp.minimum(v, w) for v, w in zip(mine, theirs[j])]
                        )
            minima = jnp.stack(list(pieces.values()))
            return row_sums(minima.reshape(ROWS_PER_DOT, KTILE), one_row[q % SUB])

        for q in range(0, groups, SUB):
            sums = one_group(q)
            for k in range(1, SUB):
                sums = sums + one_group(q + k)
            if first:
                sums = sums + part[x, pl.ds(q, SUB), :]
            part[x, pl.ds(q, SUB), :] = sums

    def add_totals(x):
        part[x, pl.ds(groups, 8), :] = own_totals
        part[x, pl.ds(groups + 1, 1), pl.ds(0, cols)] = row_sums(arrived[x])[0:1, :]

    def add_parts(x, bit):
        part_copy(x + bit, n_samp // (2 * bit)).wait_recv()
        part[x] = part[x] + part_in[x + bit]

    def chunk(i, carry):
        x = n_samp - 1 - i
        for first in range(0, samples, TREE * KTILE):
            add_unit(x, first, TREE)
        add_totals(x)
        bits = [n_samp >> k for k in range(1, n_samp.bit_length())]
        for bit in bits:
            pl.when(x < bit)(functools.partial(add_parts, x, bit))
        for bit in bits:
            @pl.when((x >= bit) & (x < 2 * bit))
            def _(bit=bit):
                part_copy(x, n_samp // (2 * bit)).start()
        pl.when((i == n_samp // 2) & (odd == 0))(functools.partial(start_pairs, reversed(range(held))))
        return carry

    lax.fori_loop(0, n_samp - 1, chunk, 0)

    for first in range(0, samples - TREE * KTILE, TREE * KTILE):
        add_unit(0, first, TREE)
    for first in range(samples - TREE * KTILE, samples, TAIL_TREE * KTILE):
        add_unit(0, first, TAIL_TREE)
    add_totals(0)
    for k in range(1, n_samp.bit_length()):
        add_parts(0, n_samp >> k)
    total_ref[...] = part[0]

    for x in range(n_samp):
        for u in range(units):
            pair_copy(x, u).wait_send()
    for x in range(1, n_samp):
        part_copy(x, 1).wait_send()
    for m in range(1, n_samp):
        next_copy(m).wait()
    own_out.wait()


def finish(
    groups, cols, total_ref, block_in, metric_hbm, block_out, metric_ref, end_sems,
):
    block_copy = pltpu.make_async_copy(block_in, block_out, end_sems.at[0])
    metric_copy = pltpu.make_async_copy(metric_ref, metric_hbm, end_sems.at[1])
    block_copy.start()
    turned = total_ref[pl.ds(0, groups), :].T
    half = cols // 2
    numerators = jnp.concatenate(
        [
            jnp.concatenate(
                [turned[part + first:part + first + half, :] for part in (0, turned.shape[0] // 2)],
                axis=0,
            )
            for first in range(0, turned.shape[0] // 2, half)
        ],
        axis=1,
    )
    own_totals = total_ref[pl.ds(groups, 1), :]
    pair_totals = total_ref[pl.ds(groups, 8), :].T[:cols, 1:2]
    metric_ref[...] = 2.0 * numerators / (own_totals + pair_totals)
    metric_copy.start()
    block_copy.wait()
    metric_copy.wait()


def fused_body(n_vblk, n_samp, vectors, partner, next_rows):
    rows, samples = vectors.shape
    cols = rows // n_samp
    groups = rows * cols // ROWS_PER_DOT
    units = samples // (TAIL_TREE * KTILE)
    part_rows = groups + 8
    next_count = next_rows.shape[0]
    hbm = pl.BlockSpec(memory_space=pl.ANY)
    dma = pltpu.SemaphoreType.DMA
    total, next_block = pl.pallas_call(
        functools.partial(kernel, n_vblk, n_samp),
        out_shape=(
            jax.ShapeDtypeStruct((part_rows, ROWS_PER_DOT), jnp.float32),
            jax.ShapeDtypeStruct((next_count * n_samp, samples), next_rows.dtype),
        ),
        in_specs=[pl.BlockSpec(memory_space=pltpu.HBM)] * 3,
        out_specs=(pl.BlockSpec(memory_space=pltpu.VMEM), hbm),
        scratch_shapes=[
            pltpu.VMEM((rows, samples), jnp.bfloat16),
            pltpu.VMEM((rows, SUB, samples), jnp.bfloat16),
            pltpu.VMEM((n_samp, cols, samples), jnp.bfloat16),
            pltpu.VMEM((next_count, samples), jnp.bfloat16),
            pltpu.VMEM((n_samp, part_rows, ROWS_PER_DOT), jnp.float32),
            pltpu.VMEM((n_samp, part_rows, ROWS_PER_DOT), jnp.float32),
            dma, dma((2,)), pltpu.SemaphoreType.REGULAR,
            dma((n_samp * units,)), dma((n_samp * units,)),
            dma((n_samp,)), dma((n_samp,)),
            dma((n_samp,)), dma((n_samp,)),
        ],
        compiler_params=pltpu.CompilerParams(
            collective_id=0, has_side_effects=True, vmem_limit_bytes=KERNEL_BYTES
        ),
        name="similarity",
    )(vectors, partner, next_rows)
    metric, next_block = pl.pallas_call(
        functools.partial(finish, groups, cols),
        out_shape=(
            jax.ShapeDtypeStruct((cols, rows), jnp.float32),
            jax.ShapeDtypeStruct(next_block.shape, next_block.dtype),
        ),
        in_specs=[pl.BlockSpec(memory_space=pltpu.VMEM)] * 2,
        out_specs=(hbm, hbm),
        scratch_shapes=[pltpu.VMEM((cols, rows), jnp.float32), dma((2,))],
        compiler_params=pltpu.CompilerParams(vmem_limit_bytes=8 * 1024 * 1024),
        name="finish",
    )(total, next_block)
    return (metric.T, next_block)


def body(n_vblk, n_samp, vectors, partner, next_rows):
    rows, samples = vectors.shape
    cols = rows // n_samp
    fits = (
        n_vblk > 2
        and n_samp > 1
        and n_samp & (n_samp - 1) == 0
        and rows == ROWS_PER_DOT
        and cols % ALIGN == 0
        and samples % (TREE * KTILE) == 0
        and next_rows.shape[0] % ALIGN == 0
        and rows * SUB * samples * 2 + 4 * rows * samples * 2 <= VMEM_BYTES
        and next_rows.shape[0] * n_samp == rows
    )
    if fits:
        return fused_body(n_vblk, n_samp, vectors, partner, next_rows)
    return plain_body(vectors, partner, next_rows)


def solution(mesh):
    in_specs = (P("vblk", "samp"), P("vblk", "samp"), P(("vblk", "samp"), None))
    out_specs = (P("vblk", "samp"), P("vblk", "samp"))
    step = functools.partial(body, mesh.shape["vblk"], mesh.shape["samp"])
    return jax.shard_map(step, mesh=mesh, in_specs=in_specs, out_specs=out_specs, check_vma=False)
```

```python
import functools

import jax
import jax.numpy as jnp
from jax import lax
from jax.experimental import pallas as pl
from jax.experimental.pallas import tpu as pltpu
from jax.sharding import PartitionSpec as P

MESH = pl.DeviceIdType.MESH
SUB = 8
ALIGN = 16
WIDTH = 256
TREE = 8
TAIL_TREE = 4
KTILE = 256
ROWS_PER_DOT = 256
VMEM_BYTES = 60 * 1024 * 1024
KERNEL_BYTES = 51712 * 1024


def from_behind(value, axis, steps):
    count = lax.axis_size(axis)
    pairs = [(source, (source + steps) % count) for source in range(count)]
    return lax.ppermute(value, axis, pairs)


def pair_terms(row_block, col_block):
    row_count = row_block.shape[0]
    grouped = row_block.reshape(row_count // 8, 8, row_block.shape[1])

    def group_sums(row_group):
        return jnp.sum(
            jnp.minimum(row_group[:, None, :], col_block[None, :, :]), axis=2, dtype=jnp.float32
        )

    numerators = lax.map(group_sums, grouped).reshape(row_count, col_block.shape[0])
    row_totals = jnp.sum(row_block, axis=1, dtype=jnp.float32)[:, None]
    col_totals = jnp.sum(col_block, axis=1, dtype=jnp.float32)[None, :]
    return (numerators, row_totals, col_totals)


def plain_body(vectors, partner, next_rows):
    next_block = lax.all_to_all(next_rows, "samp", split_axis=1, concat_axis=0, tiled=True)
    arrived = from_behind(partner, "vblk", 1)
    numerators, row_totals, col_totals = pair_terms(vectors, arrived)
    numerators, col_totals = (
        lax.psum_scatter(numerators, "samp", scatter_dimension=1, tiled=True),
        lax.psum_scatter(col_totals, "samp", scatter_dimension=1, tiled=True),
    )
    row_totals = lax.psum(row_totals, "samp")
    metric = 2.0 * numerators / (row_totals + col_totals)
    return (metric, next_block)


def flipped(index, mask, count):
    out = 0
    bit = 1
    while bit < count:
        out = out + lax.rem(lax.div(index, bit) + lax.div(mask, bit), 2) * bit
        bit *= 2
    return out


def tree_sum(values):
    while len(values) > 1:
        values = [values[i] + values[i + 1] for i in range(0, len(values), 2)]
    return values[0]


def row_sums(block, ones=None):
    if ones is None:
        ones = jnp.ones((SUB, block.shape[1]), jnp.bfloat16)
    return lax.dot_general(
        ones, block, (((1,), (1,)), ((), ())), preferred_element_type=jnp.float32
    )


def spread(slot, count):
    out = 0
    bit = 1
    while bit < count:
        out = out + lax.rem(lax.div(slot, bit), 2) * (count // (2 * bit))
        bit *= 2
    return out


def kernel(
    n_vblk, n_samp,
    vec_hbm, partner_hbm, next_hbm,
    total_ref, block_hbm,
    vec, wide, arrived, own_piece, part, part_in,
    vec_sem, piece_sem, go_sem, pair_send, pair_recv, next_send, next_recv, part_send, part_recv,
):
    b = lax.axis_index("vblk")
    s = lax.axis_index("samp")
    up = lax.rem(b + 1, n_vblk)
    down = lax.rem(b + n_vblk - 1, n_vblk)
    odd = lax.rem(s, 2)
    row_count, samples = vec.shape
    cols = row_count // n_samp
    next_count = next_hbm.shape[0]
    group = ROWS_PER_DOT // cols
    span = TAIL_TREE * KTILE
    units = samples // span

    vec_copy = pltpu.make_async_copy(vec_hbm, vec, vec_sem)
    vec_copy.start()
    own_in = pltpu.make_async_copy(
        next_hbm.at[:, pl.ds(pl.multiple_of(s * samples, samples), samples)],
        own_piece, piece_sem.at[0],
    )
    own_in.start()

    barrier = pltpu.get_barrier_semaphore()
    pl.semaphore_signal(barrier, inc=1, device_id=(down, s), device_id_type=MESH)
    for peer in range(1, n_samp, 2):
        @pl.when(s != peer)
        def _():
            pl.semaphore_signal(barrier, inc=1, device_id=(b, peer), device_id_type=MESH)
    pl.semaphore_wait(barrier, 1 + odd * (n_samp - 1))

    def pair_copy(x, u):
        owner = flipped(s, spread(x, n_samp), n_samp)
        return pltpu.make_async_remote_copy(
            src_ref=partner_hbm.at[
                pl.ds(pl.multiple_of(owner * cols, cols), cols), pl.ds(u * span, span)
            ],
            dst_ref=arrived.at[x, :, pl.ds(u * span, span)],
            send_sem=pair_send.at[x * units + u], recv_sem=pair_recv.at[x * units + u],
            device_id=(up, s), device_id_type=MESH,
        )

    def next_copy(m):
        peer = flipped(s, m or n_samp - 1, n_samp)
        first, count = {0: (next_count // 2, next_count // 2), n_samp - 1: (0, next_count // 2)}.get(
            m, (0, next_count)
        )
        rows = pl.ds(first, count)
        return pltpu.make_async_remote_copy(
            src_ref=next_hbm.at[rows, pl.ds(pl.multiple_of(peer * samples, samples), samples)],
            dst_ref=block_hbm.at[pl.ds(pl.multiple_of(s * next_count + first, ALIGN), count), :],
            send_sem=next_send.at[m], recv_sem=next_recv.at[m],
            device_id=(b, peer), device_id_type=MESH,
        )

    def part_copy(x, mask):
        return pltpu.make_async_remote_copy(
            src_ref=part.at[x], dst_ref=part_in.at[x],
            send_sem=part_send.at[x], recv_sem=part_recv.at[x],
            device_id=(b, flipped(s, mask, n_samp)), device_id_type=MESH,
        )

    def start_pairs(chunks):
        for x in chunks:
            for u in range(units):
                pair_copy(x, u).start()

    held = n_samp // 4
    order = [*range(n_samp - 1, 2, -1), 1, 2, 0]
    start_pairs(order[:n_samp - held])
    pl.when(odd == 1)(functools.partial(start_pairs, order[n_samp - held:]))

    @pl.when(odd == 1)
    def _():
        pl.semaphore_signal(go_sem, inc=1, device_id=(b, s - 1), device_id_type=MESH)

    @pl.when(odd == 0)
    def _():
        pl.semaphore_wait(go_sem, 1)

    for m in range(1, n_samp):
        next_copy(m).start()

    own_in.wait()
    own_out = pltpu.make_async_copy(
        own_piece,
        block_hbm.at[pl.ds(pl.multiple_of(s * next_count, next_count), next_count), :],
        piece_sem.at[1],
    )
    own_out.start()

    vec_copy.wait()

    def widen(t, carry):
        first = pl.multiple_of(t * ALIGN, ALIGN)
        for c in range(samples // WIDTH):
            lanes = pl.ds(c * WIDTH, WIDTH)
            rows = vec[pl.ds(first, ALIGN), lanes].astype(jnp.float32)
            for r in range(ALIGN):
                wide[first + r, :, lanes] = jnp.broadcast_to(
                    rows[r:r + 1, :], (SUB, WIDTH)
                ).astype(jnp.bfloat16)
        return carry

    lax.fori_loop(0, row_count // ALIGN, widen, 0)

    own_totals = row_sums(vec[:, pl.ds(0, KTILE)])
    own_totals = lax.fori_loop(
        1, samples // KTILE,
        lambda k, acc: acc + row_sums(vec[:, pl.ds(pl.multiple_of(k * KTILE, KTILE), KTILE)]),
        own_totals,
    )

    groups = row_count // group

    rows_of = lax.broadcasted_iota(jnp.int32, (SUB, KTILE), 0)
    one_row = [(rows_of == k).astype(jnp.bfloat16) for k in range(SUB)]

    def add_unit(x, first, tree):
        for u in range(first // span, (first + tree * KTILE) // span):
            pair_copy(x, u).wait_recv()
        at = [pl.ds(first + g * KTILE, KTILE) for g in range(tree)]

        def one_group(q):
            pieces = {}
            for half in range(2):
                js = range(half * cols // SUB // 2, (half + 1) * cols // SUB // 2)
                theirs = {j: [arrived[x, pl.ds(j * SUB, SUB), o] for o in at] for j in js}
                for r in range(group):
                    mine = [wide[r * groups + q, :, o] for o in at]
                    for j in js:
                        pieces[r, j] = tree_sum(
                            [jnp.minimum(v, w) for v, w in zip(mine, theirs[j])]
                        )
            minima = jnp.stack(list(pieces.values()))
            return row_sums(minima.reshape(ROWS_PER_DOT, KTILE), one_row[q % SUB])

        for q in range(0, groups, SUB):
            sums = one_group(q)
            for k in range(1, SUB):
                sums = sums + one_group(q + k)
            if first:
                sums = sums + part[x, pl.ds(q, SUB), :]
            part[x, pl.ds(q, SUB), :] = sums

    def add_totals(x):
        part[x, pl.ds(groups, 8), :] = own_totals
        part[x, pl.ds(groups + 1, 1), pl.ds(0, cols)] = row_sums(arrived[x])[0:1, :]

    def add_parts(x, bit):
        part_copy(x + bit, n_samp // (2 * bit)).wait_recv()
        part[x] = part[x] + part_in[x + bit]

    def chunk(i, carry):
        x = n_samp - 1 - i
        x = x + jnp.where(x == 1, 1, 0) - jnp.where(x == 2, 1, 0)
        for first in range(0, samples, TREE * KTILE):
            add_unit(x, first, TREE)
        add_totals(x)
        bits = [n_samp >> k for k in range(1, n_samp.bit_length())]
        for bit in bits:
            pl.when(x < bit)(functools.partial(add_parts, x, bit))
        for bit in bits:
            @pl.when((x >= bit) & (x < 2 * bit))
            def _(bit=bit):
                part_copy(x, n_samp // (2 * bit)).start()
        pl.when(x == 1)(lambda: next_copy(0).start())
        pl.when((i == n_samp // 2) & (odd == 0))(functools.partial(start_pairs, order[n_samp - held:]))
        return carry

    lax.fori_loop(0, n_samp - 1, chunk, 0)

    for first in range(0, samples - TREE * KTILE, TREE * KTILE):
        add_unit(0, first, TREE)
    for first in range(samples - TREE * KTILE, samples, TAIL_TREE * KTILE):
        add_unit(0, first, TAIL_TREE)
    add_totals(0)
    for k in range(1, n_samp.bit_length()):
        add_parts(0, n_samp >> k)
    total_ref[...] = part[0]

    for x in range(n_samp):
        for u in range(units):
            pair_copy(x, u).wait_send()
    for x in range(1, n_samp):
        part_copy(x, 1).wait_send()
    for m in range(n_samp):
        next_copy(m).wait()
    own_out.wait()


def finish(
    groups, cols, total_ref, block_in, metric_hbm, block_out, metric_ref, end_sems,
):
    block_copy = pltpu.make_async_copy(block_in, block_out, end_sems.at[0])
    metric_copy = pltpu.make_async_copy(metric_ref, metric_hbm, end_sems.at[1])
    block_copy.start()
    turned = total_ref[pl.ds(0, groups), :].T
    half = cols // 2
    numerators = jnp.concatenate(
        [
            jnp.concatenate(
                [turned[part + first:part + first + half, :] for part in (0, turned.shape[0] // 2)],
                axis=0,
            )
            for first in range(0, turned.shape[0] // 2, half)
        ],
        axis=1,
    )
    own_totals = total_ref[pl.ds(groups, 1), :]
    pair_totals = total_ref[pl.ds(groups, 8), :].T[:cols, 1:2]
    metric_ref[...] = 2.0 * numerators / (own_totals + pair_totals)
    metric_copy.start()
    block_copy.wait()
    metric_copy.wait()


def fused_body(n_vblk, n_samp, vectors, partner, next_rows):
    rows, samples = vectors.shape
    cols = rows // n_samp
    groups = rows * cols // ROWS_PER_DOT
    units = samples // (TAIL_TREE * KTILE)
    part_rows = groups + 8
    next_count = next_rows.shape[0]
    hbm = pl.BlockSpec(memory_space=pl.ANY)
    dma = pltpu.SemaphoreType.DMA
    total, next_block = pl.pallas_call(
        functools.partial(kernel, n_vblk, n_samp),
        out_shape=(
            jax.ShapeDtypeStruct((part_rows, ROWS_PER_DOT), jnp.float32),
            jax.ShapeDtypeStruct((next_count * n_samp, samples), next_rows.dtype),
        ),
        in_specs=[pl.BlockSpec(memory_space=pltpu.HBM)] * 3,
        out_specs=(pl.BlockSpec(memory_space=pltpu.VMEM), hbm),
        scratch_shapes=[
            pltpu.VMEM((rows, samples), jnp.bfloat16),
            pltpu.VMEM((rows, SUB, samples), jnp.bfloat16),
            pltpu.VMEM((n_samp, cols, samples), jnp.bfloat16),
            pltpu.VMEM((next_count, samples), jnp.bfloat16),
            pltpu.VMEM((n_samp, part_rows, ROWS_PER_DOT), jnp.float32),
            pltpu.VMEM((n_samp, part_rows, ROWS_PER_DOT), jnp.float32),
            dma, dma((2,)), pltpu.SemaphoreType.REGULAR,
            dma((n_samp * units,)), dma((n_samp * units,)),
            dma((n_samp,)), dma((n_samp,)),
            dma((n_samp,)), dma((n_samp,)),
        ],
        compiler_params=pltpu.CompilerParams(
            collective_id=0, has_side_effects=True, vmem_limit_bytes=KERNEL_BYTES
        ),
        name="similarity",
    )(vectors, partner, next_rows)
    metric, next_block = pl.pallas_call(
        functools.partial(finish, groups, cols),
        out_shape=(
            jax.ShapeDtypeStruct((cols, rows), jnp.float32),
            jax.ShapeDtypeStruct(next_block.shape, next_block.dtype),
        ),
        in_specs=[pl.BlockSpec(memory_space=pltpu.VMEM)] * 2,
        out_specs=(hbm, hbm),
        scratch_shapes=[pltpu.VMEM((cols, rows), jnp.float32), dma((2,))],
        compiler_params=pltpu.CompilerParams(vmem_limit_bytes=8 * 1024 * 1024),
        name="finish",
    )(total, next_block)
    return (metric.T, next_block)


def body(n_vblk, n_samp, vectors, partner, next_rows):
    rows, samples = vectors.shape
    cols = rows // n_samp
    fits = (
        n_vblk > 2
        and n_samp > 2
        and n_samp & (n_samp - 1) == 0
        and rows == ROWS_PER_DOT
        and cols % ALIGN == 0
        and samples % (TREE * KTILE) == 0
        and next_rows.shape[0] % (2 * ALIGN) == 0
        and rows * SUB * samples * 2 + 4 * rows * samples * 2 <= VMEM_BYTES
        and next_rows.shape[0] * n_samp == rows
    )
    if fits:
        return fused_body(n_vblk, n_samp, vectors, partner, next_rows)
    return plain_body(vectors, partner, next_rows)


def solution(mesh):
    in_specs = (P("vblk", "samp"), P("vblk", "samp"), P(("vblk", "samp"), None))
    out_specs = (P("vblk", "samp"), P("vblk", "samp"))
    step = functools.partial(body, mesh.shape["vblk"], mesh.shape["samp"])
    return jax.shard_map(step, mesh=mesh, in_specs=in_specs, out_specs=out_specs, check_vma=False)
```
